32 devices in a mesh: row: 8 (over z, x), col: 4 (over y, core).
Axes of the slice: x: 2, y: 2, z: 4, core: 2. Of those that a mesh axis runs over, the one named last changes fastest.
Arguments:
- density_first: bfloat16 [12288, 12288], P('row', 'col'), may hold values from -0.0068359375 to 0.0068359375
- density_second: bfloat16 [12288, 12288], P('row', 'col'), may hold values from -0.0068359375 to 0.0068359375
- basis: bfloat16 [64, 4096, 896], P(('row', 'col')), may hold values from -6 to 6
- tile_list: int32 [64, 7], P(('row', 'col')), may hold values from 0 to 95, as said below
- tile_count: int32 [64], P(('row', 'col')), may hold values from 5 to 7, as said below
- point_count: int32 [64], P(('row', 'col')), may hold values from 1024 to 4096, as said below
- offsets: float32 [3, 64, 4096], P(None, ('row', 'col')), may hold values from -5 to 5
- weights: float32 [64, 4096], P(('row', 'col')), may hold values from 0.05 to 1
- atom_of_point: int32 [64, 4096], P(('row', 'col')), may hold values from 0 to 1023, as said below
Outputs:
- density: float32 [2, 64, 4096], P(None, ('row', 'col'))
- moments: float32 [2, 9, 1024], replicated
The draws below stay inside these ranges and needn't reach their ends.
Inputs may be any that keep to these rules, and one draw needn't show every extreme that they name: `tile_list`: the 7 tile numbers of each batch are 7 consecutive numbers in some order. `tile_count`: some batch has 7. `point_count`: some batch has 4096. `atom_of_point`: the points of batch g belong to atoms (g * 16 + j) mod 1024 with j from 0 to 7.
All inputs are finite; a program needn't handle non-finite values.
Results may differ from the reference program's by a relative error of at most 0.0003.
Values may be sent and summed in bfloat16 or wider, within the bound.
A program may use at most 192 MiB of HBM per device.

```python
import math
import jax
import jax.numpy as jnp
from jax import lax

TILE = 128
NB = 12288
KT = 7
PTS = 4096
ATOMS = 1024
NT = 96
BATCHES = 64
N_ROW = 8
N_COL = 4


def lift_one(key, values, top):
    chosen = jax.random.randint(jax.random.fold_in(key, 17), (), 0, values.shape[0])
    return jnp.where(jnp.arange(values.shape[0]) == chosen, top, values).astype(jnp.int32)


def draw_tile_list(key, part):
    start_key = jax.random.fold_in(key, 3)
    order_key = jax.random.fold_in(key, 5)
    starts = jax.random.randint(start_key, (BATCHES, 1), 0, NT - KT + 1)
    order_keys = jax.random.split(order_key, BATCHES)
    orders = jax.vmap(lambda single: jax.random.permutation(single, KT))(order_keys)
    return (starts + orders).astype(jnp.int32)


def draw_tile_count(key, part):
    base = jax.random.randint(jax.random.fold_in(key, 7), (BATCHES,), KT - 2, KT + 1)
    return lift_one(key, base, KT)


def draw_point_count(key, part):
    base = jax.random.randint(jax.random.fold_in(key, 11), (BATCHES,), PTS // 4, PTS + 1)
    return lift_one(key, base, PTS)


def draw_atom_of_point(key, part):
    base = (jnp.arange(BATCHES, dtype=jnp.int32) * ATOMS // BATCHES)[:, None]
    spread = jax.random.randint(jax.random.fold_in(key, 13), (BATCHES, PTS), 0, 8)
    return ((base + spread) % ATOMS).astype(jnp.int32)


def level_of(own_key, extent, pieces, low, largest):
    def one(dim, blocks):
        steps = jax.random.uniform(jax.random.fold_in(jax.random.fold_in(own_key, 6), dim), (blocks,), jnp.float32, low / len(pieces), largest / len(pieces))
        return jnp.repeat(jnp.exp(steps), extent[dim] // blocks).reshape((-1,) + (1,) * (len(extent) - dim - 1))

    gain = one(*pieces[0])
    for cut in pieces[1:]:
        gain = gain * one(*cut)
    return gain


def normal_values(key, dims, scale, reach, pieces=(), kind=jnp.bfloat16):
    entries = jax.random.normal(key, dims, jnp.float32) * scale
    if len(pieces) > 0:
        entries = level_of(key, dims, pieces, -0.22, 0.18) * entries
    return jnp.clip(entries, min=-reach, max=reach).astype(kind)


def setup_inputs(seed: int = 0) -> dict:
    seeds = jax.random.split(jax.random.key(seed), 10)
    density_first = normal_values(seeds[0], (NB, NB), ((KT * TILE) ** 2) ** -0.5, 0.0068359375, ((0, 8), (1, 4)))
    density_second = normal_values(seeds[1], (NB, NB), ((KT * TILE) ** 2) ** -0.5, 0.0068359375, ((0, 8), (1, 4)))
    basis = normal_values(seeds[2], (BATCHES, PTS, KT * TILE), 1.0, 6.0, ((0, 32),))
    tile_list = draw_tile_list(jax.random.fold_in(seeds[9], 71), 0)
    tile_count = draw_tile_count(jax.random.fold_in(seeds[9], 71), 0)
    point_count = draw_point_count(jax.random.fold_in(seeds[9], 71), 0)
    offsets = normal_values(seeds[6], (3, BATCHES, PTS), 1.0, 5.0, ((1, 32),), jnp.float32)
    weights = jnp.clip(jnp.exp(math.log(1.0) - 2.9957323 * jax.random.uniform(seeds[7], (BATCHES, PTS), jnp.float32) ** level_of(seeds[7], (BATCHES, PTS), ((0, 32),), -0.2, 0.2)), 0.05, 1.0)
    atom_of_point = draw_atom_of_point(jax.random.fold_in(seeds[9], 71), 0)
    return dict(density_first=density_first, density_second=density_second, basis=basis, tile_list=tile_list, tile_count=tile_count, point_count=point_count, offsets=offsets, weights=weights, atom_of_point=atom_of_point)


def harmonics(offsets):
    first_axis = offsets[0]
    second_axis = offsets[1]
    third_axis = offsets[2]
    radius_sq = first_axis * first_axis + second_axis * second_axis + third_axis * third_axis
    return jnp.stack([jnp.ones_like(first_axis), first_axis, second_axis, third_axis,
                      first_axis * second_axis, second_axis * third_axis,
                      3.0 * third_axis * third_axis - radius_sq,
                      first_axis * third_axis,
                      first_axis * first_axis - second_axis * second_axis])


def storage_index(tiles, parts):
    per_part = NT // parts
    return ((tiles % parts) * per_part + tiles // parts).astype(jnp.int32)


def batch_density(stored_first, stored_second, values, tiles, live_tiles, live_points):
    inside = jnp.arange(TILE, dtype=jnp.int32)[None, :]
    rows = (storage_index(tiles, N_ROW)[:, None] * TILE + inside).reshape(-1)
    cols = (storage_index(tiles, N_COL)[:, None] * TILE + inside).reshape(-1)
    col_mask = jnp.repeat((jnp.arange(KT) < live_tiles).astype(jnp.bfloat16), TILE)
    masked = values * col_mask[None, :]
    point_mask = (jnp.arange(PTS) < live_points).astype(jnp.float32)
    results = []
    for stored in (stored_first, stored_second):
        block = stored[rows[:, None], cols[None, :]]
        product = jnp.dot(masked, block, preferred_element_type=jnp.float32)
        results.append(jnp.sum(product * masked.astype(jnp.float32), axis=1) * point_mask)
    return jnp.stack(results)


def reference(density_first, density_second, basis, tile_list, tile_count, point_count, offsets, weights, atom_of_point):
    def per_batch(inputs):
        values, tiles, live_tiles, live_points = inputs
        return batch_density(density_first, density_second, values, tiles, live_tiles, live_points)

    stacked = lax.map(per_batch, (basis, tile_list, tile_count, point_count))
    density = jnp.transpose(stacked, (1, 0, 2))
    harmonic = harmonics(offsets)
    moment_terms = density[:, None] * (weights[None, None] * harmonic[None])
    flat_terms = moment_terms.reshape(2 * 9, -1).T
    summed = jax.ops.segment_sum(flat_terms, atom_of_point.reshape(-1), num_segments=ATOMS)
    moments = summed.T.reshape(2, 9, ATOMS)
    return density, moments
```

```python
import functools

import jax
import jax.numpy as jnp
from jax import lax
from jax.experimental import pallas as pl
from jax.experimental.pallas import tpu as pltpu
from jax.sharding import PartitionSpec as P

TILE = 128
ATOMS = 1024
SPREAD = 8
TERMS = 24


def share_kernel(row_count, col_count, mine, every, held, send_sem, recv_sem, self_sem):
    peers = row_count * col_count
    me = lax.axis_index("row") * col_count + lax.axis_index("col")
    barrier = pltpu.get_barrier_semaphore()

    def device(index):
        return (index // col_count, index % col_count)

    def greet(hop, carry):
        pl.semaphore_signal(
            barrier, inc=1, device_id=device((me + hop) % peers),
            device_id_type=pl.DeviceIdType.MESH,
        )
        return carry

    def copy(hop, place):
        return pltpu.make_async_remote_copy(
            src_ref=mine,
            dst_ref=held.at[place],
            send_sem=send_sem.at[hop],
            recv_sem=recv_sem.at[hop],
            device_id=device((me + hop) % peers),
            device_id_type=pl.DeviceIdType.MESH,
        )

    def send(hop, carry):
        copy(hop, me).start()
        return carry

    def finish(hop, carry):
        copy(hop, (me + peers - hop) % peers).wait_recv()
        copy(hop, me).wait_send()
        return carry

    lax.fori_loop(1, peers, greet, 0)
    own = pltpu.make_async_copy(mine, held.at[me], self_sem)
    own.start()
    pl.semaphore_wait(barrier, peers - 1)
    lax.fori_loop(1, peers, send, 0)
    own.wait()
    lax.fori_loop(1, peers, finish, 0)
    every[...] = held[...]


def share(mine, row_count, col_count, collective_id):
    peers = row_count * col_count
    shape = (peers,) + mine.shape
    return pl.pallas_call(
        functools.partial(share_kernel, row_count, col_count),
        out_shape=jax.ShapeDtypeStruct(shape, mine.dtype),
        in_specs=[pl.BlockSpec(memory_space=pltpu.VMEM)],
        out_specs=pl.BlockSpec(memory_space=pltpu.VMEM),
        scratch_shapes=[
            pltpu.VMEM(shape, mine.dtype),
            pltpu.SemaphoreType.DMA((peers,)),
            pltpu.SemaphoreType.DMA((peers,)),
            pltpu.SemaphoreType.DMA,
        ],
        compiler_params=pltpu.CompilerParams(collective_id=collective_id, has_side_effects=True),
        name="share",
    )(mine)


def pack_kernel(row_at, col_at, first, second, out, sem):
    height, width = out.shape[2], out.shape[3]

    def issue(peer, carry):
        rows = pl.ds(pl.multiple_of(row_at[peer] * TILE, TILE), height)
        cols = pl.ds(pl.multiple_of(col_at[peer] * TILE, TILE), width)
        pltpu.make_async_copy(first.at[rows, cols], out.at[peer, 0], sem).start()
        pltpu.make_async_copy(second.at[rows, cols], out.at[peer, 1], sem).start()
        return carry

    lax.fori_loop(0, out.shape[0], issue, 0)
    pltpu.make_async_copy(out, out, sem).wait()


def pack(row_at, col_at, first, second, height, width):
    peers = row_at.shape[0]
    shape = (peers, 2, height, width)
    return pl.pallas_call(
        pack_kernel,
        out_shape=jax.ShapeDtypeStruct(shape, first.dtype),
        in_specs=[
            pl.BlockSpec(memory_space=pltpu.SMEM),
            pl.BlockSpec(memory_space=pltpu.SMEM),
            pl.BlockSpec(memory_space=pl.ANY),
            pl.BlockSpec(memory_space=pl.ANY),
        ],
        out_specs=pl.BlockSpec(memory_space=pltpu.VMEM),
        scratch_shapes=[pltpu.SemaphoreType.DMA],
        cost_estimate=pl.CostEstimate(
            flops=0, bytes_accessed=4 * peers * height * width * 2, transcendentals=0
        ),
        name="pack",
    )(row_at, col_at, first, second)


def density_kernel(
    run, batch, counts, peer_at, row_slot, col_slot, arrived, basis, geometry, atoms,
    density, moments, block, sem,
):
    step = pl.program_id(0)
    points = basis.shape[1]
    span = run * TILE
    live_tiles = counts[0]
    live_points = counts[1]

    @pl.when(step == 0)
    def _():
        def issue(index, carry):
            k = index // run
            l = index % run
            peer = peer_at[index]
            rows = pl.ds(pl.multiple_of(row_slot[k] * TILE, TILE), TILE)
            cols = pl.ds(pl.multiple_of(col_slot[l] * TILE, TILE), TILE)
            to_rows = pl.ds(pl.multiple_of(k * TILE, TILE), TILE)
            for d in range(2):
                to_cols = pl.ds(pl.multiple_of(d * span + l * TILE, TILE), TILE)
                pltpu.make_async_copy(
                    arrived.at[peer, d, rows, cols], block.at[to_rows, to_cols], sem
                ).start()
            return carry

        lax.fori_loop(0, run * run, issue, 0)
        moments[...] = jnp.zeros_like(moments)
        pltpu.make_async_copy(block, block, sem).wait()
        for k in range(run):

            @pl.when(k >= live_tiles)
            def _():
                for l in range(2 * run):
                    block[k * TILE:(k + 1) * TILE, l * TILE:(l + 1) * TILE] = jnp.zeros(
                        (TILE, TILE), block.dtype
                    )
                for d in range(2):
                    for l in range(run):
                        first = d * span + k * TILE
                        block[l * TILE:(l + 1) * TILE, first:first + TILE] = jnp.zeros(
                            (TILE, TILE), block.dtype
                        )

    @pl.when(step * points >= live_points)
    def _():
        density[...] = jnp.zeros_like(density)

    @pl.when(step * points < live_points)
    def _():
        values = basis[0]
        place = step * points + lax.broadcasted_iota(jnp.int32, (1, points), 1)
        live = place < live_points
        rows = []
        for d in range(2):
            product = jnp.dot(
                values, block[:, d * span:(d + 1) * span], preferred_element_type=jnp.float32
            )
            total = None
            for l in range(run):
                part = product[:, l * TILE:(l + 1) * TILE] * values[
                    :, l * TILE:(l + 1) * TILE
                ].astype(jnp.float32)
                total = part if total is None else total + part
            row = jnp.sum(total.T, axis=0, keepdims=True)
            rows.append(jnp.where(live, row, 0.0))
        density[...] = jnp.concatenate(rows, axis=0)
        x = geometry[0:1, :]
        y = geometry[1:2, :]
        z = geometry[2:3, :]
        w = geometry[3:4, :]
        r2 = x * x + y * y + z * z
        weighted = [
            w, w * x, w * y, w * z, w * (x * y), w * (y * z),
            w * (3.0 * z * z - r2), w * (x * z), w * (x * x - y * y),
        ]
        terms = [rows[d] * item for d in range(2) for item in weighted]
        terms += [jnp.zeros((1, points), jnp.float32)] * (TERMS - len(terms))
        stacked = jnp.concatenate(terms, axis=0)
        atom = atoms[...]
        for j in range(SPREAD):
            chosen = jnp.where(atom == j, stacked, 0.0)
            total = None
            for c in range(points // TILE):
                part = chosen[:, c * TILE:(c + 1) * TILE]
                total = part if total is None else total + part
            moments[j] = moments[j] + total


def density_of(batch, counts, peer_at, row_slot, col_slot, arrived, basis, geometry, atoms):
    points, span = basis.shape[1], basis.shape[2]
    run = span // TILE
    chunk = min(512, points)
    grid = points // chunk

    def basis_map(i, counts, *_):
        last = jnp.maximum((counts[1] + chunk - 1) // chunk - 1, 0)
        return (batch, jnp.minimum(i, last), 0)

    return pl.pallas_call(
        functools.partial(density_kernel, run, batch),
        grid_spec=pltpu.PrefetchScalarGridSpec(
            num_scalar_prefetch=4,
            grid=(grid,),
            in_specs=[
                pl.BlockSpec(memory_space=pl.ANY),
                pl.BlockSpec((1, chunk, span), basis_map),
                pl.BlockSpec((4, chunk), lambda i, *_: (0, i)),
                pl.BlockSpec((1, chunk), lambda i, *_: (0, i)),
            ],
            out_specs=[
                pl.BlockSpec((2, chunk), lambda i, *_: (0, i)),
                pl.BlockSpec((SPREAD, TERMS, TILE), lambda i, *_: (0, 0, 0)),
            ],
            scratch_shapes=[
                pltpu.VMEM((span, 2 * span), basis.dtype),
                pltpu.SemaphoreType.DMA,
            ],
        ),
        out_shape=[
            jax.ShapeDtypeStruct((2, points), jnp.float32),
            jax.ShapeDtypeStruct((SPREAD, TERMS, TILE), jnp.float32),
        ],
        compiler_params=pltpu.CompilerParams(
            dimension_semantics=("arbitrary",), vmem_limit_bytes=60 * 1024 * 1024
        ),
        cost_estimate=pl.CostEstimate(
            flops=4 * points * span * span,
            bytes_accessed=2 * points * span + 4 * span * span,
            transcendentals=0,
        ),
        name="density",
    )(counts, peer_at, row_slot, col_slot, arrived, basis, geometry, atoms)


def local(
    density_first,
    density_second,
    basis,
    tile_list,
    tile_count,
    point_count,
    offsets,
    weights,
    atom_of_point,
):
    row_count = lax.axis_size("row")
    col_count = lax.axis_size("col")
    peers = row_count * col_count
    local_rows = density_first.shape[0] // TILE
    local_cols = density_first.shape[1] // TILE
    batches_dev, run = tile_list.shape
    row_slots = min(-(-run // row_count), local_rows)
    col_slots = min(-(-run // col_count), local_cols)
    my_row = lax.axis_index("row")
    my_col = lax.axis_index("col")
    me = my_row * col_count + my_col
    own_start = jnp.min(tile_list, axis=1)
    padded = jnp.pad(own_start[:, None], ((0, -batches_dev % 8), (0, TILE - 1)))
    starts = share(padded, row_count, col_count, 0)[:, :batches_dev, 0]

    def first_held(start, owner, parts, held, slots):
        first = (start + (owner - start) % parts) // parts
        return jnp.minimum(first, held - slots).astype(jnp.int32)

    row_at = first_held(starts, my_row, row_count, local_rows, row_slots)
    col_at = first_held(starts, my_col, col_count, local_cols, col_slots)

    moved = [
        lax.all_to_all(
            pack(
                row_at[:, b], col_at[:, b], density_first, density_second,
                row_slots * TILE, col_slots * TILE,
            ),
            ("row", "col"), split_axis=0, concat_axis=0, tiled=True,
        )
        for b in range(batches_dev)
    ]

    own = own_start[:, None]
    owner_row = tile_list % row_count
    owner_col = tile_list % col_count
    row_slot = tile_list // row_count - first_held(own, owner_row, row_count, local_rows, row_slots)
    col_slot = tile_list // col_count - first_held(own, owner_col, col_count, local_cols, col_slots)
    peer_at = (owner_row[:, :, None] * col_count + owner_col[:, None, :]).reshape(batches_dev, -1)
    stride = ATOMS // (peers * batches_dev)
    base = (me * batches_dev + jnp.arange(batches_dev, dtype=jnp.int32)) * stride
    atom_slot = (atom_of_point - base[:, None]) % ATOMS
    geometry = jnp.concatenate([offsets, weights[None]], axis=0)

    densities = []
    partials = []
    for b in range(batches_dev):
        density, partial = density_of(
            b, jnp.stack([tile_count[b], point_count[b]]), peer_at[b], row_slot[b], col_slot[b],
            moved[b], basis, geometry[:, b], atom_slot[b:b + 1],
        )
        densities.append(density)
        partials.append(jnp.sum(partial, axis=2))
    density = jnp.stack(densities, axis=1)
    mine = jnp.concatenate(partials, axis=0)
    mine = jnp.pad(mine, ((0, 0), (0, TILE - TERMS)))
    every = share(mine, row_count, col_count, 1)
    every = every.reshape(peers * batches_dev, SPREAD, TILE)[:, :, :18]
    blocks = -(-SPREAD // stride)
    every = jnp.pad(every, ((0, 0), (0, blocks * stride - SPREAD), (0, 0)))
    total = None
    for q in range(blocks):
        part = every[:, q * stride:(q + 1) * stride].reshape(ATOMS, 18)
        part = jnp.roll(part, q * stride, axis=0)
        total = part if total is None else total + part
    return density, total.T.reshape(2, 9, ATOMS)


def solution(mesh):
    placed = (
        P("row", "col"),
        P("row", "col"),
        P(("row", "col"), None, None),
        P(("row", "col"), None),
        P(("row", "col")),
        P(("row", "col")),
        P(None, ("row", "col"), None),
        P(("row", "col"), None),
        P(("row", "col"), None),
    )
    return jax.shard_map(
        local,
        mesh=mesh,
        in_specs=placed,
        out_specs=(P(None, ("row", "col"), None), P()),
        check_vma=False,
    )
```

```python
import functools

import jax
import jax.numpy as jnp
from jax import lax
from jax.experimental import pallas as pl
from jax.experimental.pallas import tpu as pltpu
from jax.sharding import PartitionSpec as P

TILE = 128
ATOMS = 1024
SPREAD = 8
TERMS = 24


def share_kernel(row_count, col_count, mine, every, held, send_sem, recv_sem, self_sem):
    peers = row_count * col_count
    me = lax.axis_index("row") * col_count + lax.axis_index("col")
    barrier = pltpu.get_barrier_semaphore()

    def device(index):
        return (index // col_count, index % col_count)

    def greet(hop, carry):
        pl.semaphore_signal(
            barrier, inc=1, device_id=device((me + hop) % peers),
            device_id_type=pl.DeviceIdType.MESH,
        )
        return carry

    def copy(hop, place):
        return pltpu.make_async_remote_copy(
            src_ref=mine,
            dst_ref=held.at[place],
            send_sem=send_sem.at[hop],
            recv_sem=recv_sem.at[hop],
            device_id=device((me + hop) % peers),
            device_id_type=pl.DeviceIdType.MESH,
        )

    def send(hop, carry):
        copy(hop, me).start()
        return carry

    def finish(hop, carry):
        copy(hop, (me + peers - hop) % peers).wait_recv()
        copy(hop, me).wait_send()
        return carry

    lax.fori_loop(1, peers, greet, 0)
    own = pltpu.make_async_copy(mine, held.at[me], self_sem)
    own.start()
    pl.semaphore_wait(barrier, peers - 1)
    lax.fori_loop(1, peers, send, 0)
    own.wait()
    lax.fori_loop(1, peers, finish, 0)
    every[...] = held[...]


def share(mine, row_count, col_count, collective_id):
    peers = row_count * col_count
    shape = (peers,) + mine.shape
    return pl.pallas_call(
        functools.partial(share_kernel, row_count, col_count),
        out_shape=jax.ShapeDtypeStruct(shape, mine.dtype),
        in_specs=[pl.BlockSpec(memory_space=pltpu.VMEM)],
        out_specs=pl.BlockSpec(memory_space=pltpu.VMEM),
        scratch_shapes=[
            pltpu.VMEM(shape, mine.dtype),
            pltpu.SemaphoreType.DMA((peers,)),
            pltpu.SemaphoreType.DMA((peers,)),
            pltpu.SemaphoreType.DMA,
        ],
        compiler_params=pltpu.CompilerParams(collective_id=collective_id, has_side_effects=True),
        name="share",
    )(mine)


def pack_kernel(row_at, col_at, first, second, out, sem):
    height, width = out.shape[2], out.shape[3]

    def issue(peer, carry):
        rows = pl.ds(pl.multiple_of(row_at[peer] * TILE, TILE), height)
        cols = pl.ds(pl.multiple_of(col_at[peer] * TILE, TILE), width)
        pltpu.make_async_copy(first.at[rows, cols], out.at[peer, 0], sem).start()
        pltpu.make_async_copy(second.at[rows, cols], out.at[peer, 1], sem).start()
        return carry

    lax.fori_loop(0, out.shape[0], issue, 0)
    pltpu.make_async_copy(out, out, sem).wait()


def pack(row_at, col_at, first, second, height, width):
    peers = row_at.shape[0]
    shape = (peers, 2, height, width)
    return pl.pallas_call(
        pack_kernel,
        out_shape=jax.ShapeDtypeStruct(shape, first.dtype),
        in_specs=[
            pl.BlockSpec(memory_space=pltpu.SMEM),
            pl.BlockSpec(memory_space=pltpu.SMEM),
            pl.BlockSpec(memory_space=pl.ANY),
            pl.BlockSpec(memory_space=pl.ANY),
        ],
        out_specs=pl.BlockSpec(memory_space=pltpu.VMEM),
        scratch_shapes=[pltpu.SemaphoreType.DMA],
        cost_estimate=pl.CostEstimate(
            flops=0, bytes_accessed=4 * peers * height * width * 2, transcendentals=0
        ),
        name="pack",
    )(row_at, col_at, first, second)


def density_kernel(
    run, batch, counts, peer_at, row_slot, col_slot, arrived, basis, geometry, atoms,
    density, moments, block, sem,
):
    step = pl.program_id(0)
    points = basis.shape[1]
    span = run * TILE
    live_tiles = counts[0]
    live_points = counts[1]

    @pl.when(step == 0)
    def _():
        def issue(index, carry):
            k = index // run
            l = index % run
            peer = peer_at[index]
            rows = pl.ds(pl.multiple_of(row_slot[k] * TILE, TILE), TILE)
            cols = pl.ds(pl.multiple_of(col_slot[l] * TILE, TILE), TILE)
            to_rows = pl.ds(pl.multiple_of(k * TILE, TILE), TILE)
            for d in range(2):
                to_cols = pl.ds(pl.multiple_of(d * span + l * TILE, TILE), TILE)
                pltpu.make_async_copy(
                    arrived.at[peer, d, rows, cols], block.at[to_rows, to_cols], sem
                ).start()
            return carry

        lax.fori_loop(0, run * run, issue, 0)
        moments[...] = jnp.zeros_like(moments)
        pltpu.make_async_copy(block, block, sem).wait()
        for k in range(run):

            @pl.when(k >= live_tiles)
            def _():
                for l in range(2 * run):
                    block[k * TILE:(k + 1) * TILE, l * TILE:(l + 1) * TILE] = jnp.zeros(
                        (TILE, TILE), block.dtype
                    )
                for d in range(2):
                    for l in range(run):
                        first = d * span + k * TILE
                        block[l * TILE:(l + 1) * TILE, first:first + TILE] = jnp.zeros(
                            (TILE, TILE), block.dtype
                        )

    @pl.when(step * points >= live_points)
    def _():
        density[...] = jnp.zeros_like(density)

    @pl.when(step * points < live_points)
    def _():
        place = step * points + lax.broadcasted_iota(jnp.int32, (1, points), 1)
        live = place < live_points
        fewest = max(run - 2, 1)
        for used in range(fewest, run + 1):
            width = used * TILE

            @pl.when(live_tiles <= used if used == fewest else live_tiles == used)
            def _():
                values = basis[0, :, 0:width]
                parts = []
                for d in range(2):
                    product = jnp.dot(
                        values, block[0:width, d * span:d * span + width],
                        preferred_element_type=jnp.float32,
                    )
                    total = None
                    for l in range(used):
                        part = product[:, l * TILE:(l + 1) * TILE] * values[
                            :, l * TILE:(l + 1) * TILE
                        ].astype(jnp.float32)
                        total = part if total is None else total + part
                    row = jnp.sum(total.T, axis=0, keepdims=True)
                    parts.append(jnp.where(live, row, 0.0))
                density[...] = jnp.concatenate(parts, axis=0)

        rows = [density[d:d + 1, :] for d in range(2)]
        x = geometry[0:1, :]
        y = geometry[1:2, :]
        z = geometry[2:3, :]
        w = geometry[3:4, :]
        r2 = x * x + y * y + z * z
        weighted = [
            w, w * x, w * y, w * z, w * (x * y), w * (y * z),
            w * (3.0 * z * z - r2), w * (x * z), w * (x * x - y * y),
        ]
        terms = [rows[d] * item for d in range(2) for item in weighted]
        terms += [jnp.zeros((1, points), jnp.float32)] * (TERMS - len(terms))
        stacked = jnp.concatenate(terms, axis=0)
        atom = atoms[...]
        for j in range(SPREAD):
            chosen = jnp.where(atom == j, stacked, 0.0)
            total = None
            for c in range(points // TILE):
                part = chosen[:, c * TILE:(c + 1) * TILE]
                total = part if total is None else total + part
            moments[j] = moments[j] + total


def density_of(batch, counts, peer_at, row_slot, col_slot, arrived, basis, geometry, atoms):
    points, span = basis.shape[1], basis.shape[2]
    run = span // TILE
    chunk = min(512, points)
    grid = points // chunk

    def basis_map(i, counts, *_):
        last = jnp.maximum((counts[1] + chunk - 1) // chunk - 1, 0)
        return (batch, jnp.minimum(i, last), 0)

    return pl.pallas_call(
        functools.partial(density_kernel, run, batch),
        grid_spec=pltpu.PrefetchScalarGridSpec(
            num_scalar_prefetch=4,
            grid=(grid,),
            in_specs=[
                pl.BlockSpec(memory_space=pl.ANY),
                pl.BlockSpec((1, chunk, span), basis_map),
                pl.BlockSpec((4, chunk), lambda i, *_: (0, i)),
                pl.BlockSpec((1, chunk), lambda i, *_: (0, i)),
            ],
            out_specs=[
                pl.BlockSpec((2, chunk), lambda i, *_: (0, i)),
                pl.BlockSpec((SPREAD, TERMS, TILE), lambda i, *_: (0, 0, 0)),
            ],
            scratch_shapes=[
                pltpu.VMEM((span, 2 * span), basis.dtype),
                pltpu.SemaphoreType.DMA,
            ],
        ),
        out_shape=[
            jax.ShapeDtypeStruct((2, points), jnp.float32),
            jax.ShapeDtypeStruct((SPREAD, TERMS, TILE), jnp.float32),
        ],
        compiler_params=pltpu.CompilerParams(
            dimension_semantics=("arbitrary",), vmem_limit_bytes=60 * 1024 * 1024
        ),
        cost_estimate=pl.CostEstimate(
            flops=4 * points * span * span,
            bytes_accessed=2 * points * span + 4 * span * span,
            transcendentals=0,
        ),
        name="density",
    )(counts, peer_at, row_slot, col_slot, arrived, basis, geometry, atoms)


def local(
    density_first,
    density_second,
    basis,
    tile_list,
    tile_count,
    point_count,
    offsets,
    weights,
    atom_of_point,
):
    row_count = lax.axis_size("row")
    col_count = lax.axis_size("col")
    peers = row_count * col_count
    local_rows = density_first.shape[0] // TILE
    local_cols = density_first.shape[1] // TILE
    batches_dev, run = tile_list.shape
    row_slots = min(-(-run // row_count), local_rows)
    col_slots = min(-(-run // col_count), local_cols)
    my_row = lax.axis_index("row")
    my_col = lax.axis_index("col")
    me = my_row * col_count + my_col
    own_start = jnp.min(tile_list, axis=1)
    padded = jnp.pad(own_start[None, :], ((0, 0), (0, TILE - batches_dev)))
    starts = share(padded, row_count, col_count, 0)[:, 0, :batches_dev]

    def first_held(start, owner, parts, held, slots):
        first = (start + (owner - start) % parts) // parts
        return jnp.minimum(first, held - slots).astype(jnp.int32)

    row_at = first_held(starts, my_row, row_count, local_rows, row_slots)
    col_at = first_held(starts, my_col, col_count, local_cols, col_slots)

    moved = [
        lax.all_to_all(
            pack(
                row_at[:, b], col_at[:, b], density_first, density_second,
                row_slots * TILE, col_slots * TILE,
            ),
            ("row", "col"), split_axis=0, concat_axis=0, tiled=True,
        )
        for b in range(batches_dev)
    ]

    own = own_start[:, None]
    owner_row = tile_list % row_count
    owner_col = tile_list % col_count
    row_slot = tile_list // row_count - first_held(own, owner_row, row_count, local_rows, row_slots)
    col_slot = tile_list // col_count - first_held(own, owner_col, col_count, local_cols, col_slots)
    peer_at = (owner_row[:, :, None] * col_count + owner_col[:, None, :]).reshape(batches_dev, -1)
    stride = ATOMS // (peers * batches_dev)
    base = (me * batches_dev + jnp.arange(batches_dev, dtype=jnp.int32)) * stride
    atom_slot = (atom_of_point - base[:, None]) % ATOMS
    geometry = jnp.concatenate([offsets, weights[None]], axis=0)

    densities = []
    partials = []
    for b in range(batches_dev):
        density, partial = density_of(
            b, jnp.stack([tile_count[b], point_count[b]]), peer_at[b], row_slot[b], col_slot[b],
            moved[b], basis, geometry[:, b], atom_slot[b:b + 1],
        )
        densities.append(density)
        partials.append(jnp.sum(partial, axis=2))
    density = jnp.stack(densities, axis=1)
    mine = jnp.concatenate(partials, axis=1)
    mine = jnp.pad(mine, ((0, 0), (0, -mine.shape[1] % TILE)))
    every = share(mine, row_count, col_count, 1)
    every = jnp.stack(
        [every[:, :, b * TERMS:b * TERMS + 18] for b in range(batches_dev)], axis=1
    ).reshape(peers * batches_dev, SPREAD, 18)
    blocks = -(-SPREAD // stride)
    every = jnp.pad(every, ((0, 0), (0, blocks * stride - SPREAD), (0, 0)))
    total = None
    for q in range(blocks):
        part = every[:, q * stride:(q + 1) * stride].reshape(ATOMS, 18)
        part = jnp.roll(part, q * stride, axis=0)
        total = part if total is None else total + part
    return density, total.T.reshape(2, 9, ATOMS)


def solution(mesh):
    placed = (
        P("row", "col"),
        P("row", "col"),
        P(("row", "col"), None, None),
        P(("row", "col"), None),
        P(("row", "col")),
        P(("row", "col")),
        P(None, ("row", "col"), None),
        P(("row", "col"), None),
        P(("row", "col"), None),
    )
    return jax.shard_map(
        local,
        mesh=mesh,
        in_specs=placed,
        out_specs=(P(None, ("row", "col"), None), P()),
        check_vma=False,
    )
```
